32 devices in a mesh: blk: 4 (over x, core), vox: 8 (over z, y).
Axes of the slice: x: 2, y: 2, z: 4, core: 2. Of those that a mesh axis runs over, the one named last changes fastest.
Arguments:
- src_fields: bfloat16 [256, 32768], P('blk', 'vox'), may hold values from -6 to 6
- det_fields: bfloat16 [256, 32768], P('blk', 'vox'), may hold values from -6 to 6
- probes: bfloat16 [2, 32768], P(None, 'vox'), may hold values from -6 to 6
Outputs:
- curvature: float32 [2, 32768], P(None, 'vox')
The draws below stay inside these ranges and needn't reach their ends.
All inputs are finite; a program needn't handle non-finite values.
Results may differ from the reference program's by a relative error of at most 0.0016.
Values may be sent and summed in bfloat16 or wider, within the bound.
No kernel may reach another device: no remote copies, remote signals or barrier semaphores. Data moves between devices by JAX's collectives and lax.ppermute only.
A program may use at most 64 MiB of HBM per device.

```python
import jax
import jax.numpy as jnp
from jax import lax

PROBES = 2
VOX_DEV = 4096
SOURCES = 256
DETECTORS = 256
VOXELS = 32768
N_VOX = 8


def levels(stream_key, extent, split, low, top_value):
    def one(position, shards_of):
        heights = jax.random.uniform(jax.random.fold_in(jax.random.fold_in(stream_key, 6), position), (shards_of,), jnp.float32, low / len(split), top_value / len(split))
        return jnp.repeat(jnp.exp(heights), extent[position] // shards_of).reshape((-1,) + (1,) * (len(extent) - position - 1))

    gain = one(*split[0])
    for cut in split[1:]:
        gain = gain * one(*cut)
    return gain


def bell_draw(own_key, shape, scale, bound, shards=(), kind=jnp.bfloat16):
    values = jax.random.normal(own_key, shape, jnp.float32) * scale
    if len(shards) > 0:
        values = levels(own_key, shape, shards, -0.22, 0.18) * values
    return jnp.clip(values, min=-bound, max=bound).astype(kind)


def setup_inputs(seed: int = 0) -> dict:
    keys = jax.random.split(jax.random.key(seed), 4)
    src_fields = bell_draw(keys[0], (SOURCES, VOXELS), 1.0, 6.0, ((0, 4), (1, 8)))
    det_fields = bell_draw(keys[1], (DETECTORS, VOXELS), 1.0, 6.0, ((0, 4), (1, 8)))
    probes = bell_draw(keys[2], (PROBES, VOXELS), 1.0, 6.0, ((1, 8),))
    return {"src_fields": src_fields, "det_fields": det_fields, "probes": probes}


def reference(src_fields, det_fields, probes):
    def measure(probe_row):
        weighted = (src_fields.astype(jnp.float32) * probe_row.astype(jnp.float32)[None, :]).astype(jnp.bfloat16)
        return jnp.dot(weighted, det_fields.T, preferred_element_type=jnp.float32)

    measured = lax.map(measure, probes)
    measured_b = measured.astype(jnp.bfloat16).astype(jnp.float32)
    src_blocks = src_fields.reshape(SOURCES, N_VOX, VOX_DEV).transpose(1, 0, 2)
    det_blocks = det_fields.reshape(DETECTORS, N_VOX, VOX_DEV).transpose(1, 0, 2)

    def adjoint(pair):
        src_block, det_block = pair
        backproj = jnp.einsum("ksd,dv->ksv", measured_b, det_block.astype(jnp.float32), precision=lax.Precision.HIGHEST)
        return jnp.sum(src_block.astype(jnp.float32)[None] * backproj, axis=1)

    blocks = lax.map(adjoint, (src_blocks, det_blocks))
    total = blocks.transpose(1, 0, 2).reshape(PROBES, VOXELS)
    return total / jnp.float32(SOURCES * DETECTORS)
```

```python
import jax
import jax.numpy as jnp
from jax import lax
from jax.sharding import PartitionSpec as P


HEADROOM = 14.0
TAG_ROWS = 16
SMALLEST = 2.0**-100


def power_of_two(n):
    return n & (n - 1) == 0


def fallback(src_fields, det_fields, probes):
    src_count, vox_count = src_fields.shape
    groups = lax.axis_size("blk")
    weighted = (src_fields.astype(jnp.float32)[None] * probes.astype(jnp.float32)[:, None]).astype(jnp.bfloat16)
    weighted = weighted.reshape(-1, vox_count)
    det_all = lax.all_gather(det_fields, "blk", axis=0, tiled=True)
    product = jnp.einsum("rv,dv->rd", weighted, det_all, preferred_element_type=jnp.float32)
    measured_b = lax.psum(product, "vox").astype(jnp.bfloat16)
    backproj = jnp.dot(measured_b, det_all, preferred_element_type=jnp.float32)
    backproj = backproj.reshape(-1, src_count, vox_count)
    contrib = jnp.sum(src_fields.astype(jnp.float32)[None] * backproj, axis=1)
    normalizer = jnp.float32(1.0 / (src_count * groups * det_all.shape[0]))
    return lax.psum(contrib, "blk") * normalizer


def pack(values, exponent):
    scaled = (values * jnp.exp2(HEADROOM - exponent)).astype(jnp.float16)
    tag = jnp.broadcast_to(exponent.astype(jnp.float16), (TAG_ROWS, values.shape[1]))
    return jnp.concatenate([scaled, tag], axis=0)


def unpack(packed):
    exponent = packed[-TAG_ROWS:][:1].astype(jnp.float32)
    return packed[:-TAG_ROWS].astype(jnp.float32) * jnp.exp2(exponent - HEADROOM), exponent


def product(src_fields, det_fields, probes):
    src_count, vox_count = src_fields.shape
    det_count = det_fields.shape[0]
    probe_count = probes.shape[0]
    groups = lax.axis_size("blk")
    slabs = lax.axis_size("vox")
    if groups < 4 or not power_of_two(groups) or not power_of_two(slabs):
        return fallback(src_fields, det_fields, probes)

    def exchange(array, chip_mask, slab_mask, cross):
        pairs = []
        for b in range(groups):
            for u in range(slabs):
                core = cross if cross < 2 else u.bit_count() & 1
                pairs.append((b * slabs + u, (b ^ (2 * chip_mask) ^ core) * slabs + (u ^ slab_mask)))
        return lax.ppermute(array, ("blk", "vox"), pairs)

    others = [exchange(det_fields, m, 0, 2) for m in range(1, groups // 2)]
    partner = exchange(src_fields, 0, 0, 1)
    probe_rows = probes.astype(jnp.float32)[:, None]

    def weigh(src):
        return (src.astype(jnp.float32)[None] * probe_rows).astype(jnp.bfloat16).reshape(-1, vox_count)

    weighted = jnp.concatenate([weigh(src_fields), weigh(partner)], axis=0)
    src = jnp.concatenate([src_fields, partner], axis=0)

    def measure(det):
        return jnp.einsum("dv,rv->dr", det, weighted, preferred_element_type=jnp.float32)

    odd = lax.population_count(lax.axis_index("vox")) & 1

    def own_order(columns):
        half = columns.shape[1] // 2
        return jnp.where(odd == 1, jnp.concatenate([columns[:, half:], columns[:, :half]], axis=1), columns)

    def total_over_slabs(measured, cross):
        exponent = jnp.ceil(jnp.log2(jnp.maximum(jnp.max(jnp.abs(measured), axis=0, keepdims=True), SMALLEST)))
        width = 1
        while width < slabs:
            sent = exchange(pack(measured, exponent), 0, width, cross)
            received, other = unpack(sent)
            measured = measured + received
            exponent = jnp.maximum(exponent, other) + 1.0
            width *= 2
        return measured.astype(jnp.bfloat16)

    def project(measured_b, det):
        rows = measured_b.reshape(-1, 2, probe_count, src_count).transpose(2, 0, 1, 3).reshape(-1, 2 * src_count)
        back = jnp.dot(rows, src, preferred_element_type=jnp.float32)
        back = back.reshape(probe_count, -1, vox_count)
        return jnp.sum(det.astype(jnp.float32)[None] * back, axis=1)

    near = total_over_slabs(measure(det_fields), 0)
    total = project(near, det_fields)
    far_det = others[0] if len(others) == 1 else jnp.concatenate(others, axis=0)
    measured = own_order(measure(far_det))
    far = own_order(total_over_slabs(measured, 1))
    total = total + project(far, far_det)
    cross, mask = 1, 1
    while mask < groups // 2:
        total = total + exchange(total, mask, 0, cross)
        cross, mask = 0, 2 * mask
    total = total + exchange(total, 0, 0, 1)
    return total * jnp.float32(1.0 / (src_count * groups * det_count * groups))


def solution(mesh):
    return jax.shard_map(
        product,
        mesh=mesh,
        in_specs=(P("blk", "vox"), P("blk", "vox"), P(None, "vox")),
        out_specs=P(None, "vox"),
        check_vma=False,
    )
```

```python
import jax
import jax.numpy as jnp
from jax import lax
from jax.sharding import PartitionSpec as P


HEADROOM = 14.0
TAG_ROWS = 16
SMALLEST = 2.0**-100


def power_of_two(n):
    return n & (n - 1) == 0


def fallback(src_fields, det_fields, probes):
    src_count, vox_count = src_fields.shape
    groups = lax.axis_size("blk")
    weighted = (src_fields.astype(jnp.float32)[None] * probes.astype(jnp.float32)[:, None]).astype(jnp.bfloat16)
    weighted = weighted.reshape(-1, vox_count)
    det_all = lax.all_gather(det_fields, "blk", axis=0, tiled=True)
    product = jnp.einsum("rv,dv->rd", weighted, det_all, preferred_element_type=jnp.float32)
    measured_b = lax.psum(product, "vox").astype(jnp.bfloat16)
    backproj = jnp.dot(measured_b, det_all, preferred_element_type=jnp.float32)
    backproj = backproj.reshape(-1, src_count, vox_count)
    contrib = jnp.sum(src_fields.astype(jnp.float32)[None] * backproj, axis=1)
    normalizer = jnp.float32(1.0 / (src_count * groups * det_all.shape[0]))
    return lax.psum(contrib, "blk") * normalizer


def pack(values, exponent):
    scaled = (values * jnp.exp2(HEADROOM - exponent)).astype(jnp.float16)
    tag = jnp.broadcast_to(exponent.astype(jnp.float16), (TAG_ROWS, values.shape[1]))
    return jnp.concatenate([scaled, tag], axis=0)


def unpack(packed):
    exponent = packed[-TAG_ROWS:][:1].astype(jnp.float32)
    return packed[:-TAG_ROWS].astype(jnp.float32) * jnp.exp2(exponent - HEADROOM), exponent


def product(src_fields, det_fields, probes):
    src_count, vox_count = src_fields.shape
    det_count = det_fields.shape[0]
    probe_count = probes.shape[0]
    groups = lax.axis_size("blk")
    slabs = lax.axis_size("vox")
    if groups < 4 or not power_of_two(groups) or not power_of_two(slabs):
        return fallback(src_fields, det_fields, probes)

    def exchange(array, chip_mask, slab_mask, cross):
        pairs = []
        for b in range(groups):
            for u in range(slabs):
                core = cross if cross < 2 else u.bit_count() & 1
                pairs.append((b * slabs + u, (b ^ (2 * chip_mask) ^ core) * slabs + (u ^ slab_mask)))
        return lax.ppermute(array, ("blk", "vox"), pairs)

    others = [exchange(det_fields, m, 0, 2) for m in range(1, groups // 2)]
    partner = exchange(src_fields, 0, 0, 1)
    probe_rows = probes.astype(jnp.float32)[:, None]

    def weigh(src):
        return (src.astype(jnp.float32)[None] * probe_rows).astype(jnp.bfloat16).reshape(-1, vox_count)

    first = (lax.axis_index("blk") & 1) == 0
    src = jnp.concatenate([jnp.where(first, src_fields, partner), jnp.where(first, partner, src_fields)], axis=0)
    weighted = weigh(src)

    def measure(det):
        return jnp.einsum("dv,rv->dr", det, weighted, preferred_element_type=jnp.float32)

    def total_over_slabs(measured, cross):
        exponent = jnp.ceil(jnp.log2(jnp.maximum(jnp.max(jnp.abs(measured), axis=0, keepdims=True), SMALLEST)))
        width = 1
        while width < slabs:
            sent = exchange(pack(measured, exponent), 0, width, cross)
            received, other = unpack(sent)
            measured = measured + received
            exponent = jnp.maximum(exponent, other) + 1.0
            width *= 2
        return measured.astype(jnp.bfloat16)

    def project(measured_b, det):
        rows = measured_b.reshape(-1, probe_count, 2 * src_count).transpose(1, 0, 2).reshape(-1, 2 * src_count)
        back = jnp.dot(rows, src, preferred_element_type=jnp.float32)
        back = back.reshape(probe_count, -1, vox_count)
        return jnp.sum(det.astype(jnp.float32)[None] * back, axis=1)

    near = total_over_slabs(measure(det_fields), 0)
    total = project(near, det_fields)
    far_det = others[0] if len(others) == 1 else jnp.concatenate(others, axis=0)
    measured = measure(far_det)
    far = total_over_slabs(measured, 1)
    total = total + project(far, far_det)
    cross, mask = 1, 1
    while mask < groups // 2:
        total = total + exchange(total, mask, 0, cross)
        cross, mask = 0, 2 * mask
    total = total + exchange(total, 0, 0, 1)
    return total * jnp.float32(1.0 / (src_count * groups * det_count * groups))


def solution(mesh):
    return jax.shard_map(
        product,
        mesh=mesh,
        in_specs=(P("blk", "vox"), P("blk", "vox"), P(None, "vox")),
        out_specs=P(None, "vox"),
        check_vma=False,
    )
```

```python
import jax
import jax.numpy as jnp
from jax import lax
from jax.experimental import pallas as pl
from jax.experimental.pallas import tpu as pltpu
from jax.sharding import PartitionSpec as P


HEADROOM = 14.0
TAG_ROWS = 8
SMALLEST = 2.0**-100


def power_of_two(n):
    return n & (n - 1) == 0


def fallback(src_fields, det_fields, probes):
    src_count, vox_count = src_fields.shape
    groups = lax.axis_size("blk")
    weighted = (src_fields.astype(jnp.float32)[None] * probes.astype(jnp.float32)[:, None]).astype(jnp.bfloat16)
    weighted = weighted.reshape(-1, vox_count)
    det_all = lax.all_gather(det_fields, "blk", axis=0, tiled=True)
    product = jnp.einsum("rv,dv->rd", weighted, det_all, preferred_element_type=jnp.float32)
    measured_b = lax.psum(product, "vox").astype(jnp.bfloat16)
    backproj = jnp.dot(measured_b, det_all, preferred_element_type=jnp.float32)
    backproj = backproj.reshape(-1, src_count, vox_count)
    contrib = jnp.sum(src_fields.astype(jnp.float32)[None] * backproj, axis=1)
    normalizer = jnp.float32(1.0 / (src_count * groups * det_all.shape[0]))
    return lax.psum(contrib, "blk") * normalizer


def pack(values, exponent):
    scaled = (values * jnp.exp2(HEADROOM - exponent)).astype(jnp.float16)
    tag = jnp.broadcast_to(exponent.astype(jnp.float16), (TAG_ROWS, values.shape[1]))
    return jnp.concatenate([scaled, tag], axis=0)


def unpack(packed):
    exponent = packed[-TAG_ROWS:][:1].astype(jnp.float32)
    return packed[:-TAG_ROWS].astype(jnp.float32) * jnp.exp2(exponent - HEADROOM), exponent


def stage(*arrays):
    count = len(arrays)

    def body(*refs):
        sources, targets, sems = refs[:count], refs[count : 2 * count], refs[2 * count]
        copies = [pltpu.make_async_copy(a, b, sems.at[i]) for i, (a, b) in enumerate(zip(sources, targets))]
        for copy in copies:
            copy.start()
        for copy in copies:
            copy.wait()

    return pl.pallas_call(
        body,
        out_shape=[pltpu.VMEM(a.shape, a.dtype) for a in arrays],
        in_specs=[pl.BlockSpec(memory_space=pl.ANY)] * count,
        out_specs=[pl.BlockSpec(memory_space=pltpu.VMEM)] * count,
        scratch_shapes=[pltpu.SemaphoreType.DMA((count,))],
        name="stage",
    )(*arrays)


def product(src_fields, det_fields, probes):
    src_count, vox_count = src_fields.shape
    det_count = det_fields.shape[0]
    probe_count = probes.shape[0]
    groups = lax.axis_size("blk")
    slabs = lax.axis_size("vox")
    chips = groups // 2
    if groups < 4 or slabs < 2 or not power_of_two(groups) or not power_of_two(slabs):
        return fallback(src_fields, det_fields, probes)

    def exchange(array, partner_of):
        pairs = []
        for b in range(groups):
            for u in range(slabs):
                partner = partner_of(b // 2, b % 2, u)
                if partner is not None:
                    chip, core, slab = partner
                    pairs.append((b * slabs + u, (2 * chip + core) * slabs + slab))
        return lax.ppermute(array, ("blk", "vox"), pairs)

    def core_swap(array):
        return exchange(array, lambda q, c, u: (q, c ^ 1, u))

    def fetch(array, j, trade):
        def partner_of(q, c, u):
            if c == 1:
                return q ^ (chips // 2 + j), c, u
            if j:
                return q ^ j, c, u
            return (q, c, u ^ 1) if trade else None

        return exchange(array, partner_of)

    south = (lax.axis_index("blk") & 1) == 0
    fetched_a = [fetch(det_fields, j, True) for j in range(chips // 2)]
    det_other = core_swap(det_fields)
    src_other = core_swap(src_fields)
    fetched_b = [fetch(det_other, j, False) for j in range(chips // 2)]
    src_fields, det_fields, probes = stage(src_fields, det_fields, probes)
    probe_rows = probes.astype(jnp.float32)[:, None]
    src = jnp.concatenate([src_fields, src_other], axis=0)
    weighted = (src.astype(jnp.float32)[None] * probe_rows).astype(jnp.bfloat16).reshape(-1, vox_count)

    dets, products = [], []
    for local, fetched in ((det_fields, fetched_a), (det_other, fetched_b)):
        for j, block in enumerate(fetched):
            det = block if j else jnp.where(south, local, block)
            dets.append(det)
            products.append(jnp.einsum("dv,rv->dr", det, weighted, preferred_element_type=jnp.float32))
    measured = jnp.concatenate(products, axis=0)

    exponent = jnp.ceil(jnp.log2(jnp.maximum(jnp.max(jnp.abs(measured), axis=0, keepdims=True), SMALLEST)))
    widths = [1 << i for i in range(slabs.bit_length() - 1)]
    for width in widths[-1:] + widths[:-1]:
        sent = exchange(pack(measured, exponent), lambda q, c, u, width=width: (q, c, u ^ width))
        received, other = unpack(sent)
        measured = measured + received
        exponent = jnp.maximum(exponent, other) + 1.0
    measured_b = measured.astype(jnp.bfloat16)

    total = jnp.zeros((probe_count, vox_count), jnp.float32)
    for i, det in enumerate(dets):
        rows = measured_b[i * det_count : (i + 1) * det_count].reshape(-1, probe_count, 2 * src_count)
        rows = rows.transpose(1, 0, 2).reshape(-1, 2 * src_count)
        back = jnp.dot(rows, src, preferred_element_type=jnp.float32).reshape(probe_count, -1, vox_count)
        total = total + jnp.sum(det.astype(jnp.float32)[None] * back, axis=1)
    total = total + core_swap(total)
    mask = 1
    while mask < chips:
        total = total + exchange(total, lambda q, c, u, mask=mask: (q ^ mask, c ^ 1, u))
        mask *= 2
    return total * jnp.float32(1.0 / (src_count * groups * det_count * groups))


def solution(mesh):
    return jax.shard_map(
        product,
        mesh=mesh,
        in_specs=(P("blk", "vox"), P("blk", "vox"), P(None, "vox")),
        out_specs=P(None, "vox"),
        check_vma=False,
    )
```

```python
import jax
import jax.numpy as jnp
from jax import lax
from jax.experimental import pallas as pl
from jax.experimental.pallas import tpu as pltpu
from jax.sharding import PartitionSpec as P


HEADROOM = 14.0
TAG_ROWS = 8
SMALLEST = 2.0**-100


def power_of_two(n):
    return n & (n - 1) == 0


def fallback(src_fields, det_fields, probes):
    src_count, vox_count = src_fields.shape
    groups = lax.axis_size("blk")
    weighted = (src_fields.astype(jnp.float32)[None] * probes.astype(jnp.float32)[:, None]).astype(jnp.bfloat16)
    weighted = weighted.reshape(-1, vox_count)
    det_all = lax.all_gather(det_fields, "blk", axis=0, tiled=True)
    product = jnp.einsum("rv,dv->rd", weighted, det_all, preferred_element_type=jnp.float32)
    measured_b = lax.psum(product, "vox").astype(jnp.bfloat16)
    backproj = jnp.dot(measured_b, det_all, preferred_element_type=jnp.float32)
    backproj = backproj.reshape(-1, src_count, vox_count)
    contrib = jnp.sum(src_fields.astype(jnp.float32)[None] * backproj, axis=1)
    normalizer = jnp.float32(1.0 / (src_count * groups * det_all.shape[0]))
    return lax.psum(contrib, "blk") * normalizer


def pack(values, exponent):
    scaled = (values * jnp.exp2(HEADROOM - exponent)).astype(jnp.float16)
    tag = jnp.broadcast_to(exponent.astype(jnp.float16), (TAG_ROWS, values.shape[1]))
    return jnp.concatenate([scaled, tag], axis=0)


def unpack(packed):
    exponent = packed[-TAG_ROWS:][:1].astype(jnp.float32)
    return packed[:-TAG_ROWS].astype(jnp.float32) * jnp.exp2(exponent - HEADROOM), exponent


def stage(*arrays):
    count = len(arrays)

    def body(*refs):
        sources, targets, sems = refs[:count], refs[count : 2 * count], refs[2 * count]
        copies = [pltpu.make_async_copy(a, b, sems.at[i]) for i, (a, b) in enumerate(zip(sources, targets))]
        for copy in copies:
            copy.start()
        for copy in copies:
            copy.wait()

    return pl.pallas_call(
        body,
        out_shape=[pltpu.VMEM(a.shape, a.dtype) for a in arrays],
        in_specs=[pl.BlockSpec(memory_space=pl.ANY)] * count,
        out_specs=[pl.BlockSpec(memory_space=pltpu.VMEM)] * count,
        scratch_shapes=[pltpu.SemaphoreType.DMA((count,))],
        name="stage",
    )(*arrays)


def choose_product(local_first, local, det, weighted):
    def body(flag, local_ref, det_ref, weighted_ref, out_ref):
        @pl.when(flag[0] == 1)
        def _():
            out_ref[...] = local_ref[...]

        @pl.when(flag[0] == 0)
        def _():
            out_ref[...] = lax.dot_general(
                det_ref[...], weighted_ref[...], (((1,), (1,)), ((), ())), preferred_element_type=jnp.float32
            )

    vmem = pl.BlockSpec(memory_space=pltpu.VMEM)
    return pl.pallas_call(
        body,
        out_shape=pltpu.VMEM(local.shape, local.dtype),
        in_specs=[pl.BlockSpec(memory_space=pltpu.SMEM), vmem, vmem, vmem],
        out_specs=vmem,
        compiler_params=pltpu.CompilerParams(vmem_limit_bytes=8 << 20),
        name="choose_product",
    )(local_first, *(pltpu.with_memory_space_constraint(x, pltpu.VMEM) for x in (local, det, weighted)))


def product(src_fields, det_fields, probes):
    src_count, vox_count = src_fields.shape
    det_count = det_fields.shape[0]
    probe_count = probes.shape[0]
    groups = lax.axis_size("blk")
    slabs = lax.axis_size("vox")
    chips = groups // 2
    if groups < 4 or slabs < 2 or not power_of_two(groups) or not power_of_two(slabs):
        return fallback(src_fields, det_fields, probes)

    def exchange(array, partner_of):
        pairs = []
        for b in range(groups):
            for u in range(slabs):
                partner = partner_of(b // 2, b % 2, u)
                if partner is not None:
                    chip, core, slab = partner
                    pairs.append((b * slabs + u, (2 * chip + core) * slabs + slab))
        return lax.ppermute(array, ("blk", "vox"), pairs)

    def core_swap(array):
        return exchange(array, lambda q, c, u: (q, c ^ 1, u))

    def fetch(array, j, trade):
        def partner_of(q, c, u):
            if c == 1:
                return q ^ (chips // 2 + j), c, u
            if j:
                return q ^ j, c, u
            return (q, c, u ^ 1) if trade else None

        return exchange(array, partner_of)

    south = (lax.axis_index("blk") & 1) == 0
    fetched_a = [fetch(det_fields, j, True) for j in range(chips // 2)]
    det_other = core_swap(det_fields)
    src_other = core_swap(src_fields)
    fetched_b = [fetch(det_other, j, False) for j in range(chips // 2)]
    src_fields, det_fields, probes = stage(src_fields, det_fields, probes)
    probe_rows = probes.astype(jnp.float32)[:, None]
    src = jnp.concatenate([src_fields, src_other], axis=0)
    weighted = (src.astype(jnp.float32)[None] * probe_rows).astype(jnp.bfloat16).reshape(-1, vox_count)

    def measure(det):
        return jnp.einsum("dv,rv->dr", det, weighted, preferred_element_type=jnp.float32)

    flag = south.astype(jnp.int32).reshape(1)
    dets, products = [], []
    for local, fetched in ((det_fields, fetched_a), (det_other, fetched_b)):
        local_product = measure(local)
        for j, block in enumerate(fetched):
            if j:
                dets.append(block)
                products.append(measure(block))
            else:
                dets.append(jnp.where(south, local, block))
                products.append(choose_product(flag, local_product, block, weighted))
    measured = jnp.concatenate(products, axis=0)

    exponent = jnp.ceil(jnp.log2(jnp.maximum(jnp.max(jnp.abs(measured), axis=0, keepdims=True), SMALLEST)))
    widths = [1 << i for i in range(slabs.bit_length() - 1)]
    for width in widths[-1:] + widths[:-1]:
        sent = exchange(pack(measured, exponent), lambda q, c, u, width=width: (q, c, u ^ width))
        received, other = unpack(sent)
        measured = measured + received
        exponent = jnp.maximum(exponent, other) + 1.0
    measured_b = measured.astype(jnp.bfloat16)

    total = jnp.zeros((probe_count, vox_count), jnp.float32)
    for i, det in enumerate(dets):
        rows = measured_b[i * det_count : (i + 1) * det_count].reshape(-1, probe_count, 2 * src_count)
        rows = rows.transpose(1, 0, 2).reshape(-1, 2 * src_count)
        back = jnp.dot(rows, src, preferred_element_type=jnp.float32).reshape(probe_count, -1, vox_count)
        total = total + jnp.sum(det.astype(jnp.float32)[None] * back, axis=1)
    mask = 1
    while mask < chips:
        total = total + exchange(total, lambda q, c, u, mask=mask: (q ^ mask, c, u))
        mask *= 2
    total = total + core_swap(total)
    return total * jnp.float32(1.0 / (src_count * groups * det_count * groups))


def solution(mesh):
    return jax.shard_map(
        product,
        mesh=mesh,
        in_specs=(P("blk", "vox"), P("blk", "vox"), P(None, "vox")),
        out_specs=P(None, "vox"),
        check_vma=False,
    )
```

```python
import jax
import jax.numpy as jnp
from jax import lax
from jax.experimental import pallas as pl
from jax.experimental.pallas import tpu as pltpu
from jax.sharding import PartitionSpec as P


HEADROOM = 14.0
TAG_ROWS = 8
SMALLEST = 2.0**-100
CHUNK = 512


def power_of_two(n):
    return n & (n - 1) == 0


def fallback(src_fields, det_fields, probes):
    src_count, vox_count = src_fields.shape
    groups = lax.axis_size("blk")
    weighted = (src_fields.astype(jnp.float32)[None] * probes.astype(jnp.float32)[:, None]).astype(jnp.bfloat16)
    weighted = weighted.reshape(-1, vox_count)
    det_all = lax.all_gather(det_fields, "blk", axis=0, tiled=True)
    product = jnp.einsum("rv,dv->rd", weighted, det_all, preferred_element_type=jnp.float32)
    measured_b = lax.psum(product, "vox").astype(jnp.bfloat16)
    backproj = jnp.dot(measured_b, det_all, preferred_element_type=jnp.float32)
    backproj = backproj.reshape(-1, src_count, vox_count)
    contrib = jnp.sum(src_fields.astype(jnp.float32)[None] * backproj, axis=1)
    normalizer = jnp.float32(1.0 / (src_count * groups * det_all.shape[0]))
    return lax.psum(contrib, "blk") * normalizer


def pack(values, exponent):
    scaled = (values * jnp.exp2(HEADROOM - exponent)).astype(jnp.float16)
    tag = jnp.broadcast_to(exponent.astype(jnp.float16), (TAG_ROWS, values.shape[1]))
    return jnp.concatenate([scaled, tag], axis=0)


def unpack(packed):
    exponent = packed[-TAG_ROWS:][:1].astype(jnp.float32)
    return packed[:-TAG_ROWS].astype(jnp.float32) * jnp.exp2(exponent - HEADROOM), exponent


def stage(*arrays):
    count = len(arrays)

    def body(*refs):
        sources, targets, sems = refs[:count], refs[count : 2 * count], refs[2 * count]
        copies = [pltpu.make_async_copy(a, b, sems.at[i]) for i, (a, b) in enumerate(zip(sources, targets))]
        for copy in copies:
            copy.start()
        for copy in copies:
            copy.wait()

    return pl.pallas_call(
        body,
        out_shape=[pltpu.VMEM(a.shape, a.dtype) for a in arrays],
        in_specs=[pl.BlockSpec(memory_space=pl.ANY)] * count,
        out_specs=[pl.BlockSpec(memory_space=pltpu.VMEM)] * count,
        scratch_shapes=[pltpu.SemaphoreType.DMA((count,))],
        name="stage",
    )(*arrays)


def in_vmem(body, shape, dtype, *arrays, flags=()):
    vmem = pl.BlockSpec(memory_space=pltpu.VMEM)
    return pl.pallas_call(
        body,
        out_shape=pltpu.VMEM(shape, dtype),
        in_specs=[pl.BlockSpec(memory_space=pltpu.SMEM)] * len(flags) + [vmem] * len(arrays),
        out_specs=vmem,
        compiler_params=pltpu.CompilerParams(vmem_limit_bytes=16 << 20),
    )(*flags, *(pltpu.with_memory_space_constraint(x, pltpu.VMEM) for x in arrays))


def chunks(extent):
    size = min(extent, CHUNK)
    return [slice(i, min(i + size, extent)) for i in range(0, extent, size)]


def weigh(src, probes):
    count, extent = src.shape

    def body(src_ref, probes_ref, out_ref):
        for cut in chunks(extent):
            values = src_ref[:, cut].astype(jnp.float32)
            for k in range(probes.shape[0]):
                weighted = (values * probes_ref[k : k + 1, cut].astype(jnp.float32)).astype(jnp.bfloat16)
                out_ref[cut, k * count : (k + 1) * count] = weighted.T

    return in_vmem(body, (extent, probes.shape[0] * count), jnp.bfloat16, src, probes)


def choose_product(local_first, local, det, weighted):
    def body(flag, local_ref, det_ref, weighted_ref, out_ref):
        @pl.when(flag[0] == 1)
        def _():
            out_ref[...] = local_ref[...]

        @pl.when(flag[0] == 0)
        def _():
            out_ref[...] = jnp.dot(det_ref[...], weighted_ref[...], preferred_element_type=jnp.float32)

    return in_vmem(body, local.shape, local.dtype, local, det, weighted, flags=(local_first,))


def project(measured_b, src, dets, probe_count):
    count, extent = src.shape

    def body(measured_ref, src_ref, *refs):
        det_refs, out_ref = refs[:-1], refs[-1]
        rows = [measured_ref[:, k * count : (k + 1) * count] for k in range(probe_count)]
        rows = jnp.concatenate(rows, axis=0)
        for cut in chunks(extent):
            back = jnp.dot(rows, src_ref[:, cut], preferred_element_type=jnp.float32)
            first = 0
            for k in range(probe_count):
                total = 0.0
                for det_ref in det_refs:
                    last = first + det_ref.shape[0]
                    total = total + jnp.sum(back[first:last] * det_ref[:, cut].astype(jnp.float32), axis=0, keepdims=True)
                    first = last
                out_ref[k : k + 1, cut] = total

    return in_vmem(body, (probe_count, extent), jnp.float32, measured_b, src, *dets)


def product(src_fields, det_fields, probes):
    src_count, _ = src_fields.shape
    det_count = det_fields.shape[0]
    probe_count = probes.shape[0]
    groups = lax.axis_size("blk")
    slabs = lax.axis_size("vox")
    chips = groups // 2
    if groups < 4 or slabs < 2 or not power_of_two(groups) or not power_of_two(slabs):
        return fallback(src_fields, det_fields, probes)

    def exchange(array, partner_of):
        pairs = []
        for b in range(groups):
            for u in range(slabs):
                partner = partner_of(b // 2, b % 2, u)
                if partner is not None:
                    chip, core, slab = partner
                    pairs.append((b * slabs + u, (2 * chip + core) * slabs + slab))
        return lax.ppermute(array, ("blk", "vox"), pairs)

    def core_swap(array):
        return exchange(array, lambda q, c, u: (q, c ^ 1, u))

    def fetch(array, j, trade):
        def partner_of(q, c, u):
            if c == 1:
                return q ^ (chips // 2 + j), c, u
            if j:
                return q ^ j, c, u
            return (q, c, u ^ 1) if trade else None

        return exchange(array, partner_of)

    south = (lax.axis_index("blk") & 1) == 0
    fetched_a = [fetch(det_fields, j, True) for j in range(chips // 2)]
    det_other = core_swap(det_fields)
    src_other = core_swap(src_fields)
    fetched_b = [fetch(det_other, j, False) for j in range(chips // 2)]
    src_fields, det_fields, probes = stage(src_fields, det_fields, probes)
    src = jnp.concatenate([src_fields, src_other], axis=0)
    weighted = weigh(src, probes)

    def measure(det):
        return jnp.dot(det, weighted, preferred_element_type=jnp.float32)

    flag = south.astype(jnp.int32).reshape(1)
    dets, products = [], []
    for local, fetched in ((det_fields, fetched_a), (det_other, fetched_b)):
        local_product = measure(local)
        for j, block in enumerate(fetched):
            if j:
                dets.append(block)
                products.append(measure(block))
            else:
                dets.append(jnp.where(south, local, block))
                products.append(choose_product(flag, local_product, block, weighted))
    measured = jnp.concatenate(products, axis=0)

    exponent = jnp.ceil(jnp.log2(jnp.maximum(jnp.max(jnp.abs(measured), axis=0, keepdims=True), SMALLEST)))
    widths = [1 << i for i in range(slabs.bit_length() - 1)]
    for width in widths[-1:] + widths[:-1]:
        sent = exchange(pack(measured, exponent), lambda q, c, u, width=width: (q, c, u ^ width))
        received, other = unpack(sent)
        measured = measured + received
        exponent = jnp.maximum(exponent, other) + 1.0
    measured_b = measured.astype(jnp.bfloat16)

    total = project(measured_b, src, dets, probe_count)
    mask = 1
    while mask < chips:
        total = total + exchange(total, lambda q, c, u, mask=mask: (q ^ mask, c, u))
        mask *= 2
    total = total + core_swap(total)
    return total * jnp.float32(1.0 / (src_count * groups * det_count * groups))


def solution(mesh):
    return jax.shard_map(
        product,
        mesh=mesh,
        in_specs=(P("blk", "vox"), P("blk", "vox"), P(None, "vox")),
        out_specs=P(None, "vox"),
        check_vma=False,
    )
```

```python
import jax
import jax.numpy as jnp
from jax import lax
from jax.experimental import pallas as pl
from jax.experimental.pallas import tpu as pltpu
from jax.sharding import PartitionSpec as P


HEADROOM = 14.0
TAG_ROWS = 8
SMALLEST = 2.0**-100
CHUNK = 512


def power_of_two(n):
    return n & (n - 1) == 0


def fallback(src_fields, det_fields, probes):
    src_count, vox_count = src_fields.shape
    groups = lax.axis_size("blk")
    weighted = (src_fields.astype(jnp.float32)[None] * probes.astype(jnp.float32)[:, None]).astype(jnp.bfloat16)
    weighted = weighted.reshape(-1, vox_count)
    det_all = lax.all_gather(det_fields, "blk", axis=0, tiled=True)
    product = jnp.einsum("rv,dv->rd", weighted, det_all, preferred_element_type=jnp.float32)
    measured_b = lax.psum(product, "vox").astype(jnp.bfloat16)
    backproj = jnp.dot(measured_b, det_all, preferred_element_type=jnp.float32)
    backproj = backproj.reshape(-1, src_count, vox_count)
    contrib = jnp.sum(src_fields.astype(jnp.float32)[None] * backproj, axis=1)
    normalizer = jnp.float32(1.0 / (src_count * groups * det_all.shape[0]))
    return lax.psum(contrib, "blk") * normalizer


def pack(values, exponent):
    scaled = (values * jnp.exp2(HEADROOM - exponent)).astype(jnp.float16)
    tag = jnp.broadcast_to(exponent.astype(jnp.float16), (TAG_ROWS, values.shape[1]))
    return jnp.concatenate([scaled, tag], axis=0)


def unpack(packed):
    exponent = packed[-TAG_ROWS:][:1].astype(jnp.float32)
    return packed[:-TAG_ROWS].astype(jnp.float32) * jnp.exp2(exponent - HEADROOM), exponent


def stage(*arrays):
    count = len(arrays)

    def body(*refs):
        sources, targets, sems = refs[:count], refs[count : 2 * count], refs[2 * count]
        copies = [pltpu.make_async_copy(a, b, sems.at[i]) for i, (a, b) in enumerate(zip(sources, targets))]
        for copy in copies:
            copy.start()
        for copy in copies:
            copy.wait()

    return pl.pallas_call(
        body,
        out_shape=[pltpu.VMEM(a.shape, a.dtype) for a in arrays],
        in_specs=[pl.BlockSpec(memory_space=pl.ANY)] * count,
        out_specs=[pl.BlockSpec(memory_space=pltpu.VMEM)] * count,
        scratch_shapes=[pltpu.SemaphoreType.DMA((count,))],
        name="stage",
    )(*arrays)


def in_vmem(body, shape, dtype, *arrays, flags=()):
    vmem = pl.BlockSpec(memory_space=pltpu.VMEM)
    return pl.pallas_call(
        body,
        out_shape=pltpu.VMEM(shape, dtype),
        in_specs=[pl.BlockSpec(memory_space=pltpu.SMEM)] * len(flags) + [vmem] * len(arrays),
        out_specs=vmem,
        compiler_params=pltpu.CompilerParams(vmem_limit_bytes=16 << 20),
    )(*flags, *(pltpu.with_memory_space_constraint(x, pltpu.VMEM) for x in arrays))


def chunks(extent):
    size = min(extent, CHUNK)
    return [slice(i, min(i + size, extent)) for i in range(0, extent, size)]


def weigh(src, probes):
    count, extent = src.shape

    def body(src_ref, probes_ref, out_ref):
        for cut in chunks(extent):
            values = src_ref[:, cut].astype(jnp.float32)
            for k in range(probes.shape[0]):
                weighted = (values * probes_ref[k : k + 1, cut].astype(jnp.float32)).astype(jnp.bfloat16)
                out_ref[cut, k * count : (k + 1) * count] = weighted.T

    return in_vmem(body, (extent, probes.shape[0] * count), jnp.bfloat16, src, probes)


def choose_product(local_first, local, det, weighted):
    def body(flag, local_ref, det_ref, weighted_ref, out_ref):
        @pl.when(flag[0] == 1)
        def _():
            out_ref[...] = local_ref[...]

        @pl.when(flag[0] == 0)
        def _():
            out_ref[...] = jnp.dot(det_ref[...], weighted_ref[...], preferred_element_type=jnp.float32)

    return in_vmem(body, local.shape, local.dtype, local, det, weighted, flags=(local_first,))


def finish_product(local_first, local, det, weighted, earlier):
    rows, columns = earlier.shape
    total_rows = rows + local.shape[0]

    def body(flag, local_ref, det_ref, weighted_ref, earlier_ref, out_ref, exponent_ref):
        out_ref[:rows, :] = earlier_ref[...]

        @pl.when(flag[0] == 1)
        def _():
            out_ref[rows:, :] = local_ref[...]

        @pl.when(flag[0] == 0)
        def _():
            out_ref[rows:, :] = jnp.dot(det_ref[...], weighted_ref[...], preferred_element_type=jnp.float32)

        largest = jnp.max(jnp.abs(out_ref[...]), axis=0, keepdims=True)
        exponent = jnp.ceil(jnp.log2(jnp.maximum(largest, SMALLEST)))
        exponent_ref[...] = jnp.broadcast_to(exponent, exponent_ref.shape)

    vmem = pl.BlockSpec(memory_space=pltpu.VMEM)
    return pl.pallas_call(
        body,
        out_shape=[pltpu.VMEM((total_rows, columns), jnp.float32), pltpu.VMEM((TAG_ROWS, columns), jnp.float32)],
        in_specs=[pl.BlockSpec(memory_space=pltpu.SMEM)] + [vmem] * 4,
        out_specs=[vmem, vmem],
        compiler_params=pltpu.CompilerParams(vmem_limit_bytes=16 << 20),
        name="choose_product",
    )(local_first, *(pltpu.with_memory_space_constraint(x, pltpu.VMEM) for x in (local, det, weighted, earlier)))


def project(measured_b, src, dets, probe_count):
    count, extent = src.shape

    def body(measured_ref, src_ref, *refs):
        det_refs, out_ref = refs[:-1], refs[-1]
        rows = [measured_ref[:, k * count : (k + 1) * count] for k in range(probe_count)]
        rows = jnp.concatenate(rows, axis=0)
        for cut in chunks(extent):
            back = jnp.dot(rows, src_ref[:, cut], preferred_element_type=jnp.float32)
            first = 0
            for k in range(probe_count):
                total = 0.0
                for det_ref in det_refs:
                    last = first + det_ref.shape[0]
                    total = total + jnp.sum(back[first:last] * det_ref[:, cut].astype(jnp.float32), axis=0, keepdims=True)
                    first = last
                out_ref[k : k + 1, cut] = total

    return in_vmem(body, (probe_count, extent), jnp.float32, measured_b, src, *dets)


def product(src_fields, det_fields, probes):
    src_count, _ = src_fields.shape
    det_count = det_fields.shape[0]
    probe_count = probes.shape[0]
    groups = lax.axis_size("blk")
    slabs = lax.axis_size("vox")
    chips = groups // 2
    if groups < 4 or slabs < 2 or not power_of_two(groups) or not power_of_two(slabs):
        return fallback(src_fields, det_fields, probes)

    def exchange(array, partner_of):
        pairs = []
        for b in range(groups):
            for u in range(slabs):
                partner = partner_of(b // 2, b % 2, u)
                if partner is not None:
                    chip, core, slab = partner
                    pairs.append((b * slabs + u, (2 * chip + core) * slabs + slab))
        return lax.ppermute(array, ("blk", "vox"), pairs)

    def core_swap(array):
        return exchange(array, lambda q, c, u: (q, c ^ 1, u))

    def fetch(array, j, trade):
        def partner_of(q, c, u):
            if c == 1:
                return q ^ (chips // 2 + j), c, u
            if j:
                return q ^ j, c, u
            return (q, c, u ^ 1) if trade else None

        return exchange(array, partner_of)

    south = (lax.axis_index("blk") & 1) == 0
    fetched_a = [fetch(det_fields, j, True) for j in range(chips // 2)]
    det_other = core_swap(det_fields)
    src_other = core_swap(src_fields)
    fetched_b = [fetch(det_other, j, False) for j in range(chips // 2)]
    src_fields, det_fields, probes = stage(src_fields, det_fields, probes)
    src = jnp.concatenate([src_fields, src_other], axis=0)
    weighted = weigh(src, probes)

    def measure(det):
        return jnp.dot(det, weighted, preferred_element_type=jnp.float32)

    flag = south.astype(jnp.int32).reshape(1)
    dets, products = [], []
    for label, local, fetched in (("a", det_fields, fetched_a), ("b", det_other, fetched_b)):
        local_product = measure(local)
        for j, block in enumerate(fetched):
            if j:
                dets.append(block)
                products.append(measure(block))
                exponent = None
            else:
                dets.append(jnp.where(south, local, block))
                if label == "b":
                    earlier = products[0] if len(products) == 1 else jnp.concatenate(products, axis=0)
                    measured, exponent = finish_product(flag, local_product, block, weighted, earlier)
                    exponent, products = exponent[:1], [measured]
                else:
                    products.append(choose_product(flag, local_product, block, weighted))
    measured = products[0] if len(products) == 1 else jnp.concatenate(products, axis=0)

    if exponent is None:
        exponent = jnp.ceil(jnp.log2(jnp.maximum(jnp.max(jnp.abs(measured), axis=0, keepdims=True), SMALLEST)))
    widths = [1 << i for i in range(slabs.bit_length() - 1)]
    for width in widths[-1:] + widths[:-1]:
        sent = exchange(pack(measured, exponent), lambda q, c, u, width=width: (q, c, u ^ width))
        received, other = unpack(sent)
        measured = measured + received
        exponent = jnp.maximum(exponent, other) + 1.0
    measured_b = measured.astype(jnp.bfloat16)

    total = project(measured_b, src, dets, probe_count)
    mask = 1
    while mask < chips:
        total = total + exchange(total, lambda q, c, u, mask=mask: (q ^ mask, c, u))
        mask *= 2
    total = total + core_swap(total)
    return total * jnp.float32(1.0 / (src_count * groups * det_count * groups))


def solution(mesh):
    return jax.shard_map(
        product,
        mesh=mesh,
        in_specs=(P("blk", "vox"), P("blk", "vox"), P(None, "vox")),
        out_specs=P(None, "vox"),
        check_vma=False,
    )
```
